32 devices in a mesh: grp: 1, tok: 32 (over z, y, x, core).
Axes of the slice: x: 2, y: 2, z: 4, core: 2. Of those that a mesh axis runs over, the one named last changes fastest.
Arguments:
- queries: bfloat16 [4096, 2048], P(('grp', 'tok')), may hold values from -16 to 16
- keys: bfloat16 [4096, 2048], P(('grp', 'tok')), may hold values from -16 to 16
- values: bfloat16 [4096, 2048], P(('grp', 'tok')), may hold values from -6 to 6
- segment: int32 [4096], P(('grp', 'tok')), may hold values from 0 to 41, never falling along the last dimension, each value on 1 to 256 neighbouring positions
- rates: float32 [4096, 2], P(('grp', 'tok')), may hold values from 0.00046875 to 0.0046875
- fast_one: bfloat16 [2048, 512], P(('grp', 'tok')), may hold values from -0.1875 to 0.1875
- fast_three: bfloat16 [2048, 512], P(('grp', 'tok')), may hold values from -0.1875 to 0.1875
- fast_two: bfloat16 [2048, 512], P(('grp', 'tok')), may hold values from -0.25 to 0.25
Outputs:
- attended: bfloat16 [4096, 2048], P(('grp', 'tok'))
- fast_out: bfloat16 [4096, 2048], P(('grp', 'tok'))
The draws below stay inside these ranges and needn't reach their ends.
Inputs may be any that keep to these rules, and one draw needn't show every extreme that they name: `segment`: exemplar numbers never fall along the tokens; each exemplar covers 1 to 256 consecutive tokens.
All inputs are finite; a program needn't handle non-finite values.
Results may differ from the reference program's by a relative error of at most 0.0084.
Values may be sent and summed in bfloat16 or wider, within the bound.
A program may use at most 128 MiB of HBM per device.

```python
import math
import jax
import jax.numpy as jnp
import numpy as np
from jax import lax

D = 2048
ATT_HEADS = 16
FAST_HEADS = 2
FAST_DIM = 1024
FAST_HID = 512
WINDOW = 128
TOKENS = 4096
SEGS = 42
SEG_MOST = 256


def paired_rows(key):
    base = jax.random.fold_in(key, 7)
    key_q, key_k = jax.random.split(base, 2)
    queries = jnp.clip(jax.random.normal(key_q, (TOKENS, D), jnp.float32), -6.0, 6.0)
    keys = jnp.clip(jax.random.normal(key_k, (TOKENS, D), jnp.float32), -6.0, 6.0)
    return (queries, keys)


def draw_queries(key, part):
    return paired_rows(key)[0].astype(jnp.bfloat16)


def draw_keys(key, part):
    return paired_rows(key)[1].astype(jnp.bfloat16)


def shard_levels(key, extent, shards, least, high):
    factor_of, own = 1.0, jax.random.fold_in(key, 6)
    for dim, blocks in shards:
        steps = jnp.exp(jax.random.uniform(jax.random.fold_in(own, dim), (blocks,), jnp.float32, least / len(shards), high / len(shards)))
        factor_of = factor_of * jnp.repeat(steps, extent[dim] // blocks).reshape([-1 if axis == dim else 1 for axis in range(len(extent))])
    return factor_of


def profile(amount, total, bound, skew):
    portions = [(1 << 20) // math.isqrt(standing ** skew) + 1 for standing in range(2, amount + 1)]
    rest, given = total - bound - (amount - 1), [1] * (amount - 1)
    while rest > 0:
        candidates = [i for i in range(amount - 1) if given[i] < bound]
        whole, left = sum([portions[i] for i in candidates]), rest
        for i in candidates:
            extra = min(bound - given[i], max(1, left * portions[i] // whole), rest)
            given[i] = given[i] + extra
            rest = rest - extra
    return np.array([bound] + given)


def ragged_sizes(rng, amount, total, reach, skew):
    if amount == 2:
        one = jax.random.randint(rng, (), max(1, total - reach), min(reach, total - 1) + 1)
        return jnp.stack([one, total - one])
    tallies = jnp.asarray(profile(amount, total, reach, skew), jnp.int32)
    couples = (amount - 1) // 2
    donor, taker = tallies[1:1 + 2 * couples:2], tallies[2:2 + 2 * couples:2]
    room = jnp.minimum(donor - 1, reach - taker)
    moved = jax.random.randint(jax.random.fold_in(rng, 1), (couples,), 0, 1 << 20) % (room + 1)
    tallies = tallies.at[1:1 + 2 * couples:2].set(donor - moved).at[2:2 + 2 * couples:2].set(taker + moved)
    return tallies[jax.random.permutation(jax.random.fold_in(rng, 2), amount)]


def noise(stream_key, shape, scale, reach, cuts=(), kind=jnp.bfloat16):
    entries = jax.random.normal(stream_key, shape, jnp.float32) * scale
    if len(cuts) > 0:
        entries = shard_levels(stream_key, shape, cuts, -0.22, 0.18) * entries
    return jnp.clip(entries, min=-reach, max=reach).astype(kind)


def setup_inputs(seed: int = 0, part: int = 0) -> dict:
    key_list = jax.random.split(jax.random.key(seed), 9)
    part_splits = jax.random.split(jax.random.fold_in(key_list[8], part), 9)
    queries = draw_queries(jax.random.fold_in(jax.random.fold_in(key_list[8], part), 71), part)
    keys = draw_keys(jax.random.fold_in(jax.random.fold_in(key_list[8], part), 71), part)
    values = noise(part_splits[2], (TOKENS, D), 1.0, 6.0, ((0, 32),))
    segment = jnp.searchsorted(jnp.cumsum(ragged_sizes(part_splits[3], SEGS, TOKENS, SEG_MOST, 1)), jnp.arange(TOKENS), side="right").astype(jnp.int32)
    rates = jnp.clip(jnp.exp(math.log(0.0046875) - 2.3025852 * jax.random.uniform(part_splits[4], (TOKENS, FAST_HEADS), jnp.float32) ** shard_levels(part_splits[4], (TOKENS, FAST_HEADS), ((0, 32),), -0.2, 0.2)), 0.00046875, 0.0046875)
    fast_one = noise(part_splits[5], (FAST_HEADS * FAST_DIM, FAST_HID), FAST_DIM ** -0.5, 0.1875, ((0, 32),))
    fast_three = noise(part_splits[6], (FAST_HEADS * FAST_DIM, FAST_HID), FAST_DIM ** -0.5, 0.1875, ((0, 32),))
    fast_two = noise(part_splits[7], (FAST_HEADS * FAST_DIM, FAST_HID), FAST_HID ** -0.5, 0.25, ((0, 32),))
    return dict(queries=queries, keys=keys, values=values, segment=segment, rates=rates, fast_one=fast_one, fast_three=fast_three, fast_two=fast_two)


EPS = 1e-06

def attend(queries, keys, values, segment):
    head_dim = D // ATT_HEADS
    scale = 1.0 / math.sqrt(head_dim)
    blocks = queries.shape[0] // WINDOW
    pad_keys = jnp.concatenate([jnp.zeros((WINDOW, D), keys.dtype), keys], 0)
    pad_values = jnp.concatenate([jnp.zeros((WINDOW, D), values.dtype), values], 0)
    pad_seg = jnp.concatenate([jnp.full((WINDOW,), -1, jnp.int32), segment.astype(jnp.int32)], 0)

    def one_block(index):
        start = (index * WINDOW).astype(jnp.int32)
        q_blk = lax.dynamic_slice_in_dim(queries, start, WINDOW, 0)
        k_blk = lax.dynamic_slice_in_dim(pad_keys, start, 2 * WINDOW, 0)
        v_blk = lax.dynamic_slice_in_dim(pad_values, start, 2 * WINDOW, 0)
        s_blk = lax.dynamic_slice_in_dim(pad_seg, start, 2 * WINDOW, 0)
        s_own = lax.dynamic_slice_in_dim(segment.astype(jnp.int32), start, WINDOW, 0)
        qh = q_blk.reshape(WINDOW, ATT_HEADS, head_dim).astype(jnp.float32)
        kh = k_blk.reshape(2 * WINDOW, ATT_HEADS, head_dim).astype(jnp.float32)
        vh = v_blk.reshape(2 * WINDOW, ATT_HEADS, head_dim).astype(jnp.float32)
        scores = jnp.einsum('qhd,khd->hqk', qh, kh) * scale
        rows = jnp.arange(WINDOW, dtype=jnp.int32)[:, None] + WINDOW
        cols = jnp.arange(2 * WINDOW, dtype=jnp.int32)[None, :]
        allowed = (cols <= rows) & (rows - cols < WINDOW) & (s_blk[None, :] == s_own[:, None])
        masked = jnp.where(allowed[None], scores, jnp.float32(-1e+30))
        top = lax.optimization_barrier(jnp.max(masked, axis=2, keepdims=True))
        expo = jnp.where(allowed[None], jnp.exp(masked - top), jnp.float32(0.0))
        probs = (expo / lax.optimization_barrier(jnp.sum(expo, axis=2, keepdims=True))).astype(jnp.bfloat16)
        out = jnp.einsum('hqk,khd->qhd', probs.astype(jnp.float32), vh)
        return out.reshape(WINDOW, D).astype(jnp.bfloat16)
    outs = lax.map(one_block, jnp.arange(blocks, dtype=jnp.int32))
    return outs.reshape(blocks * WINDOW, D)

def heads_apply(rows, weight):
    grouped = rows.reshape(rows.shape[0], FAST_HEADS, FAST_DIM).astype(jnp.float32)
    matrix = weight.reshape(FAST_HEADS, FAST_DIM, FAST_HID).astype(jnp.float32)
    return jnp.einsum('thd,hdc->thc', grouped, matrix)

def outer_sum(rows, hidden):
    grouped = rows.reshape(rows.shape[0], FAST_HEADS, FAST_DIM).astype(jnp.float32)
    return jnp.einsum('thd,thc->hdc', grouped, hidden.astype(jnp.float32))

def renorm(weight, grad):
    matrix = weight.reshape(FAST_HEADS, FAST_DIM, FAST_HID).astype(jnp.float32)
    update = matrix - grad
    old_len = jnp.sqrt(lax.optimization_barrier(jnp.sum(matrix * matrix, axis=1)))
    new_len = jnp.sqrt(lax.optimization_barrier(jnp.sum(update * update, axis=1)) + EPS)
    return (update * (old_len / new_len)[:, None, :]).astype(jnp.bfloat16)

def reference(queries, keys, values, segment, rates, fast_one, fast_three, fast_two):
    attended = attend(queries, keys, values, segment)
    width = FAST_HEADS * FAST_DIM
    key_fast = keys[:, :width]
    value_fast = values[:, :width]
    query_fast = queries[:, :width]
    rate = rates.astype(jnp.float32)[:, :, None]
    a_one = heads_apply(key_fast, fast_one)
    a_three = heads_apply(key_fast, fast_three)
    sig = jax.nn.sigmoid(a_one)
    weighted = (-rate * a_one * sig * a_three).astype(jnp.bfloat16)
    grad_two = outer_sum(value_fast, weighted)
    back = -rate * heads_apply(value_fast, fast_two)
    delta_one = (back * a_three * sig * (1.0 + a_one * (1.0 - sig))).astype(jnp.bfloat16)
    delta_three = (back * a_one * sig).astype(jnp.bfloat16)
    grad_one = outer_sum(key_fast, delta_one)
    grad_three = outer_sum(key_fast, delta_three)
    new_one = renorm(fast_one, grad_one)
    new_three = renorm(fast_three, grad_three)
    new_two = renorm(fast_two, grad_two)
    grouped = query_fast.reshape(query_fast.shape[0], FAST_HEADS, FAST_DIM).astype(jnp.float32)
    b_one = jnp.einsum('thd,hdc->thc', grouped, new_one.astype(jnp.float32))
    b_three = jnp.einsum('thd,hdc->thc', grouped, new_three.astype(jnp.float32))
    mixed = (jax.nn.silu(b_one) * b_three).astype(jnp.bfloat16)
    fast_out = jnp.einsum('thc,hdc->thd', mixed.astype(jnp.float32), new_two.astype(jnp.float32))
    fast_out = fast_out.reshape(query_fast.shape[0], width).astype(jnp.bfloat16)
    return (attended, fast_out)
```

```python
import functools
import math

import jax
import jax.numpy as jnp
from jax import lax
from jax.experimental import pallas as pl
from jax.experimental.pallas import tpu as pltpu
from jax.sharding import PartitionSpec as P

D = 2048
ATT_HEADS = 16
FAST_HEADS = 2
FAST_DIM = 1024
FAST_HID = 512
WINDOW = 128


EPS = 1e-06


def from_behind(value, axis, steps):
    count = lax.axis_size(axis)
    initial, last = (max(0, -steps), min(count, count - steps))
    return lax.ppermute(value, axis, [(source, source + steps) for source in range(initial, last)])


def axis_orders(count):
    bits = count.bit_length() - 1
    rest = list(range(1, bits))
    return [[0] + rest[m:] + rest[:m] if rest else [0] for m in range(3)]


def bit_of(index, bit):
    return lax.rem(lax.div(index, jnp.int32(1 << bit)), jnp.int32(2))


def block_of(index, order):
    total = jnp.int32(0)
    for bit in order:
        total = total * 2 + bit_of(index, bit)
    return total


def device_of(block, order):
    index = 0
    for place, bit in enumerate(reversed(order)):
        index += ((block >> place) & 1) << bit
    return index


def greet(me, bits):
    barrier = pltpu.get_barrier_semaphore()
    for bit in range(bits):
        pl.semaphore_signal(
            barrier,
            inc=1,
            device_id={"tok": partner_of(me, bit)},
            device_id_type=pl.DeviceIdType.MESH,
        )
    pl.semaphore_wait(barrier, bits)


def partner_of(me, bit):
    return me + (1 - 2 * bit_of(me, bit)) * (1 << bit)


def remote(src, dst, send_sem, recv_sem, partner):
    return pltpu.make_async_remote_copy(
        src_ref=src,
        dst_ref=dst,
        send_sem=send_sem,
        recv_sem=recv_sem,
        device_id={"tok": partner},
        device_id_type=pl.DeviceIdType.MESH,
    )


def gather_kernel(count, *refs):
    orders = axis_orders(count)
    bits = count.bit_length() - 1
    parts, outs = refs[:3], refs[3:6]
    held, local_sem, send_sem, recv_sem = refs[6:]
    me = lax.axis_index("tok")
    own = [block_of(me, orders[m]) for m in range(3)]
    local = [
        pltpu.make_async_copy(parts[m], held.at[m, own[m]], local_sem.at[m]) for m in range(3)
    ]
    for copy in local:
        copy.start()
    greet(me, bits)
    copies = {}

    def send(m, step):
        bit = orders[m][bits - 1 - step]
        size = 1 << step
        start = lax.div(own[m], jnp.int32(size)) * size
        here = held.at[m, pl.ds(start, size)]
        copies[m, step] = remote(
            here, here, send_sem.at[m, step], recv_sem.at[m, step], partner_of(me, bit)
        )
        copies[m, step].start()

    for m in range(3):
        local[m].wait()
        send(m, 0)
    for step in range(bits):
        for m in range(3):
            copies[m, step].wait_recv()
            if step + 1 < bits:
                send(m, step + 1)
            else:
                for block in range(count):
                    outs[m][device_of(block, orders[m])] = held[m, block]
    for copy in copies.values():
        copy.wait_send()


def gather_weights(weights, count):
    rows, cols = weights[0].shape
    bits = count.bit_length() - 1
    outs = pl.pallas_call(
        functools.partial(gather_kernel, count),
        out_shape=[jax.ShapeDtypeStruct((count, rows, cols), jnp.bfloat16)] * 3,
        in_specs=[pl.BlockSpec(memory_space=pltpu.VMEM)] * 3,
        out_specs=[pl.BlockSpec(memory_space=pltpu.VMEM)] * 3,
        scratch_shapes=[
            pltpu.VMEM((3, count, rows, cols), jnp.bfloat16),
            pltpu.SemaphoreType.DMA((3,)),
            pltpu.SemaphoreType.DMA((3, bits)),
            pltpu.SemaphoreType.DMA((3, bits)),
        ],
        compiler_params=pltpu.CompilerParams(collective_id=0, has_side_effects=True),
        cost_estimate=pl.CostEstimate(flops=0, bytes_accessed=100_000_000, transcendentals=0),
    )(*weights)
    return [out.reshape(count * rows, cols) for out in outs]


def update_kernel(count, *refs):
    orders = axis_orders(count)
    bits = count.bit_length() - 1
    grads, olds, outs = refs[:3], refs[3:6], refs[6:9]
    total, landed, send_sem, recv_sem = refs[9:]
    me = lax.axis_index("tok")
    own = [block_of(me, orders[m]) for m in range(3)]
    greet(me, bits)
    copies = {}

    def first_kept(m, step):
        size = count >> (step + 1)
        return lax.div(own[m], jnp.int32(size)) * size

    def half_start(m):
        return lax.div(own[m], jnp.int32(count // 2)) * (count // 2)

    def send_half(m, step):
        bit = orders[m][step]
        size = count >> (step + 1)
        keep = first_kept(m, step)
        away = keep + (1 - 2 * bit_of(me, bit)) * size
        if step == 0:
            src = grads[m].at[pl.ds(away, size)]
        else:
            src = total.at[m, pl.ds(away - half_start(m), size)]
        dst = landed.at[m, pl.ds(count - 2 * size, size)]
        copies[m, step] = remote(
            src, dst, send_sem.at[m, step], recv_sem.at[m, step], partner_of(me, bit)
        )
        copies[m, step].start()

    def send_new(m, step):
        bit = orders[m][bits - 1 - step]
        size = 1 << step
        start = lax.div(own[m], jnp.int32(size)) * size
        here = outs[m].at[pl.ds(start, size)]
        at = bits + step
        copies[m, at] = remote(
            here, here, send_sem.at[m, at], recv_sem.at[m, at], partner_of(me, bit)
        )
        copies[m, at].start()

    def add_half(m, step):
        size = count >> (step + 1)
        keep = first_kept(m, step)
        offset = keep - half_start(m)

        def one(i, carry):
            mine = grads[m][keep + i] if step == 0 else total[m, offset + i]
            other = landed[m, count - 2 * size + i]
            both = mine.astype(jnp.float32) + other.astype(jnp.float32)
            total[m, offset + i] = both.astype(jnp.bfloat16)
            return carry

        lax.fori_loop(0, size, one, 0)

    for m in range(3):
        send_half(m, 0)
    for step in range(bits - 1):
        for m in range(3):
            copies[m, step].wait_recv()
            add_half(m, step)
            send_half(m, step + 1)
    for m in range(3):
        copies[m, bits - 1].wait_recv()
        mine = total[m, own[m] - half_start(m)] if bits > 1 else grads[m][own[m]]
        grad = mine.astype(jnp.float32) + landed[m, count - 2].astype(jnp.float32)
        old = olds[m][...].astype(jnp.float32)
        update = old - grad
        old_len = jnp.sqrt(jnp.sum(old * old, axis=1, keepdims=True))
        new_len = jnp.sqrt(jnp.sum(update * update, axis=1, keepdims=True) + EPS)
        outs[m][own[m]] = (update * (old_len / new_len)).astype(jnp.bfloat16)
        send_new(m, 0)
    for step in range(bits):
        for m in range(3):
            copies[m, bits + step].wait_recv()
            if step + 1 < bits:
                send_new(m, step + 1)
    for copy in copies.values():
        copy.wait_send()


def update_weights(grads, olds, count):
    rows, cols = olds[0].shape
    bits = count.bit_length() - 1
    shape = (count, rows, cols)
    return pl.pallas_call(
        functools.partial(update_kernel, count),
        out_shape=[jax.ShapeDtypeStruct(shape, jnp.bfloat16)] * 3,
        in_specs=[pl.BlockSpec(memory_space=pltpu.VMEM)] * 6,
        out_specs=[pl.BlockSpec(memory_space=pltpu.VMEM)] * 3,
        scratch_shapes=[
            pltpu.VMEM((3, count // 2, rows, cols), jnp.bfloat16),
            pltpu.VMEM((3, count, rows, cols), jnp.bfloat16),
            pltpu.SemaphoreType.DMA((3, 2 * bits)),
            pltpu.SemaphoreType.DMA((3, 2 * bits)),
        ],
        compiler_params=pltpu.CompilerParams(collective_id=1, has_side_effects=True),
        cost_estimate=pl.CostEstimate(flops=0, bytes_accessed=200_000_000, transcendentals=0),
    )(*[grad.reshape(shape) for grad in grads], *olds)


def project(rows, weight):
    matrix = weight.reshape(FAST_HEADS, FAST_DIM, weight.shape[1])
    return jnp.einsum("thd,hdc->thc", rows, matrix, preferred_element_type=jnp.float32)


def outer_sum(hidden, rows):
    summed = jnp.einsum("thc,thd->hcd", hidden, rows, preferred_element_type=jnp.float32)
    return summed.astype(jnp.bfloat16).reshape(FAST_HEADS * FAST_HID, FAST_DIM)


def per_device(queries, keys, values, segment, rates, fast_one, fast_three, fast_two):
    count = queries.shape[0]
    devices = lax.axis_size("tok")
    shard = lax.axis_index("tok")
    head_dim = D // ATT_HEADS
    scale = 1.0 / math.sqrt(head_dim)
    seg_low = (segment % 256).astype(jnp.bfloat16)
    prev_keys, prev_values, prev_seg = from_behind((keys, values, seg_low), "tok", 1)
    all_keys = jnp.concatenate([prev_keys, keys], 0)
    all_values = jnp.concatenate([prev_values, values], 0)
    all_seg = jnp.concatenate([prev_seg, seg_low], 0)
    rows = shard * count + jnp.arange(count, dtype=jnp.int32)
    cols = shard * count - count + jnp.arange(2 * count, dtype=jnp.int32)
    allowed = (cols[None, :] <= rows[:, None]) & (rows[:, None] - cols[None, :] < WINDOW)
    allowed = allowed & (cols[None, :] >= 0) & (all_seg[None, :] == seg_low[:, None])
    q_heads = queries.reshape(count, ATT_HEADS, head_dim)
    k_heads = all_keys.reshape(2 * count, ATT_HEADS, head_dim)
    v_heads = all_values.reshape(2 * count, ATT_HEADS, head_dim)
    scores = (
        jnp.einsum("qhd,khd->hqk", q_heads, k_heads, preferred_element_type=jnp.float32) * scale
    )
    masked = jnp.where(allowed[None], scores, jnp.float32(-1e30))
    top = jnp.max(masked, axis=2, keepdims=True)
    expo = jnp.where(allowed[None], jnp.exp(masked - top), jnp.float32(0.0))
    probs = (expo / jnp.sum(expo, axis=2, keepdims=True)).astype(jnp.bfloat16)
    attended = jnp.einsum("hqk,khd->qhd", probs, v_heads, preferred_element_type=jnp.float32)
    attended = attended.reshape(count, D).astype(jnp.bfloat16)
    width = FAST_HEADS * FAST_DIM
    key_fast = keys.reshape(count, FAST_HEADS, FAST_DIM)
    value_fast = values.reshape(count, FAST_HEADS, FAST_DIM)
    query_fast = queries.reshape(count, FAST_HEADS, FAST_DIM)
    fulls = gather_weights((fast_one, fast_three, fast_two), devices)
    full_one, full_three, full_two = fulls
    rate = rates[:, :, None]
    a_one = project(key_fast, full_one)
    a_three = project(key_fast, full_three)
    sig = jax.nn.sigmoid(a_one)
    weighted = (-rate * a_one * sig * a_three).astype(jnp.bfloat16)
    back = -rate * project(value_fast, full_two)
    delta_one = (back * a_three * sig * (1.0 + a_one * (1.0 - sig))).astype(jnp.bfloat16)
    delta_three = (back * a_one * sig).astype(jnp.bfloat16)
    grads = (
        outer_sum(delta_one, key_fast),
        outer_sum(delta_three, key_fast),
        outer_sum(weighted, value_fast),
    )
    rows_here = FAST_HEADS * FAST_HID // devices
    olds = []
    for m, order in enumerate(axis_orders(devices)):
        start = block_of(shard, order) * rows_here
        own_cols = lax.dynamic_slice(
            fulls[m].reshape(FAST_HEADS, FAST_DIM, FAST_HID),
            (start // FAST_HID, jnp.int32(0), start % FAST_HID),
            (1, FAST_DIM, rows_here),
        )
        olds.append(own_cols[0].T)
    news = update_weights(grads, olds, devices)
    new_one, new_three, new_two = [n.reshape(FAST_HEADS, FAST_HID, FAST_DIM) for n in news]
    b_one = jnp.einsum("thd,hcd->thc", query_fast, new_one, preferred_element_type=jnp.float32)
    b_three = jnp.einsum("thd,hcd->thc", query_fast, new_three, preferred_element_type=jnp.float32)
    mixed = (jax.nn.silu(b_one) * b_three).astype(jnp.bfloat16)
    fast_out = jnp.einsum("thc,hcd->thd", mixed, new_two, preferred_element_type=jnp.float32)
    fast_out = fast_out.reshape(count, width).astype(jnp.bfloat16)
    return (attended, fast_out)


def solution(mesh):
    placed = (
        P(("grp", "tok"), None),
        P(("grp", "tok"), None),
        P(("grp", "tok"), None),
        P(("grp", "tok")),
        P(("grp", "tok"), None),
        P(("grp", "tok"), None),
        P(("grp", "tok"), None),
        P(("grp", "tok"), None),
    )
    return jax.shard_map(
        per_device,
        mesh=mesh,
        in_specs=placed,
        out_specs=(P(("grp", "tok"), None), P(("grp", "tok"), None)),
        check_vma=False,
    )
```

```python
import functools
import math

import jax
import jax.numpy as jnp
from jax import lax
from jax.experimental import pallas as pl
from jax.experimental.pallas import tpu as pltpu
from jax.sharding import PartitionSpec as P

D = 2048
ATT_HEADS = 16
FAST_HEADS = 2
FAST_DIM = 1024
FAST_HID = 512
WINDOW = 128


EPS = 1e-06


def axis_orders(count):
    bits = count.bit_length() - 1
    rest = list(range(1, bits))
    return [[0] + rest[m:] + rest[:m] if rest else [0] for m in range(3)]


def bit_of(index, bit):
    return lax.rem(lax.div(index, jnp.int32(1 << bit)), jnp.int32(2))


def coordinate(index, bit, bits):
    here = bit_of(index, bit)
    if bits >= 3 and bit == bits - 2:
        top = bit_of(index, bits - 1)
        here = here + top - 2 * here * top
    return here


def partner_of(me, bit, bits):
    other = me + (1 - 2 * bit_of(me, bit)) * (1 << bit)
    if bits >= 3 and bit == bits - 1:
        other = other + (1 - 2 * bit_of(me, bit - 1)) * (1 << (bit - 1))
    return other


def block_of(index, order):
    total = jnp.int32(0)
    for bit in order:
        total = total * 2 + coordinate(index, bit, len(order))
    return total


def device_of(block, order):
    bits = len(order)
    index = 0
    for place, bit in enumerate(reversed(order)):
        index += ((block >> place) & 1) << bit
    if bits >= 3 and (index >> (bits - 1)) & 1:
        index ^= 1 << (bits - 2)
    return index


def greet(me, bits, others=()):
    barrier = pltpu.get_barrier_semaphore()
    partners = [partner_of(me, bit, bits) for bit in range(bits)] + list(others)
    for partner in partners:
        pl.semaphore_signal(
            barrier,
            inc=1,
            device_id={"tok": partner},
            device_id_type=pl.DeviceIdType.MESH,
        )
    pl.semaphore_wait(barrier, len(partners))


def remote(src, dst, send_sem, recv_sem, partner):
    return pltpu.make_async_remote_copy(
        src_ref=src,
        dst_ref=dst,
        send_sem=send_sem,
        recv_sem=recv_sem,
        device_id={"tok": partner},
        device_id_type=pl.DeviceIdType.MESH,
    )


def gather_kernel(count, *refs):
    orders = axis_orders(count)
    bits = count.bit_length() - 1
    parts = refs[:3]
    q_ref, k_ref, v_ref, seg_col, seg_row = refs[3:8]
    outs, att_ref = refs[8:11], refs[11]
    held, old_k, old_v, old_seg, local_sem, send_sem, recv_sem, halo_send, halo_recv = refs[12:]
    me = lax.axis_index("tok")
    after, before = lax.rem(me + 1, count), lax.rem(me + count - 1, count)
    own = [block_of(me, orders[m]) for m in range(3)]
    local = [
        pltpu.make_async_copy(parts[m], held.at[m, own[m]], local_sem.at[m]) for m in range(3)
    ]
    for copy in local:
        copy.start()
    greet(me, bits, (after, before))
    copies = {}

    def send(m, step):
        bit = orders[m][bits - 1 - step]
        size = 1 << step
        start = lax.div(own[m], jnp.int32(size)) * size
        here = held.at[m, pl.ds(start, size)]
        copies[m, step] = remote(
            here, here, send_sem.at[m, step], recv_sem.at[m, step], partner_of(me, bit, bits)
        )
        copies[m, step].start()

    for m in range(3):
        local[m].wait()
        send(m, 0)
    halo = [
        remote(src, dst, halo_send.at[i], halo_recv.at[i], after)
        for i, (src, dst) in enumerate(((seg_row, old_seg), (k_ref, old_k), (v_ref, old_v)))
    ]
    for copy in halo:
        copy.start()

    rows = q_ref.shape[0]
    dim = D // ATT_HEADS
    scale = 1.0 / math.sqrt(dim)

    def attend_heads(first, last):
        row = lax.broadcasted_iota(jnp.int32, (rows, rows), 0)
        col = lax.broadcasted_iota(jnp.int32, (rows, rows), 1)
        own_seg = seg_col[...]
        now_ok = (col <= row) & (row - col < WINDOW) & (own_seg == seg_row[0:1, :])
        old_ok = (row - col + rows < WINDOW) & (own_seg == old_seg[0:1, :]) & (row + me * rows >= row + rows)

        def one(head, carry):
            lanes = pl.ds(pl.multiple_of(head * dim, dim), dim)
            q = q_ref[:, lanes]

            def score(keys, allowed):
                dots = lax.dot_general(
                    q, keys, (((1,), (1,)), ((), ())), preferred_element_type=jnp.float32
                )
                return jnp.where(allowed, dots * scale, jnp.float32(-1e30))

            old, now = score(old_k[:, lanes], old_ok), score(k_ref[:, lanes], now_ok)
            top = jnp.maximum(
                jnp.max(old, axis=1, keepdims=True), jnp.max(now, axis=1, keepdims=True)
            )
            old = jnp.where(old_ok, jnp.exp(old - top), jnp.float32(0.0))
            now = jnp.where(now_ok, jnp.exp(now - top), jnp.float32(0.0))
            total = jnp.sum(old, axis=1, keepdims=True) + jnp.sum(now, axis=1, keepdims=True)
            out = jnp.dot(
                (old / total).astype(jnp.bfloat16),
                old_v[:, lanes],
                preferred_element_type=jnp.float32,
            ) + jnp.dot(
                (now / total).astype(jnp.bfloat16),
                v_ref[:, lanes],
                preferred_element_type=jnp.float32,
            )
            att_ref[:, lanes] = out.astype(jnp.bfloat16)
            return carry

        lax.fori_loop(first, last, one, 0)

    for step in range(bits):
        if step == bits - 2:
            for copy in halo:
                copy.wait_recv()
            attend_heads(0, 6)
        if step == bits - 1:
            attend_heads(6, ATT_HEADS)
        for m in range(3):
            copies[m, step].wait_recv()
            if step + 1 < bits:
                send(m, step + 1)
            else:
                for block in range(count):
                    outs[m][device_of(block, orders[m])] = held[m, block]
    for copy in list(copies.values()) + halo:
        copy.wait_send()


def gather_weights(weights, queries, keys, values, segment, count):
    rows, cols = weights[0].shape
    tokens = queries.shape[0]
    bits = count.bit_length() - 1
    seg_row = jnp.broadcast_to(segment[None, :], (8, tokens))
    outs = pl.pallas_call(
        functools.partial(gather_kernel, count),
        out_shape=[jax.ShapeDtypeStruct((count, rows, cols), jnp.bfloat16)] * 3
        + [jax.ShapeDtypeStruct(queries.shape, jnp.bfloat16)],
        in_specs=[pl.BlockSpec(memory_space=pltpu.VMEM)] * 8,
        out_specs=[pl.BlockSpec(memory_space=pltpu.VMEM)] * 4,
        scratch_shapes=[
            pltpu.VMEM((3, count, rows, cols), jnp.bfloat16),
            pltpu.VMEM(keys.shape, jnp.bfloat16),
            pltpu.VMEM(values.shape, jnp.bfloat16),
            pltpu.VMEM((8, tokens), jnp.int32),
            pltpu.SemaphoreType.DMA((3,)),
            pltpu.SemaphoreType.DMA((3, bits)),
            pltpu.SemaphoreType.DMA((3, bits)),
            pltpu.SemaphoreType.DMA((3,)),
            pltpu.SemaphoreType.DMA((3,)),
        ],
        compiler_params=pltpu.CompilerParams(collective_id=0, has_side_effects=True),
        cost_estimate=pl.CostEstimate(flops=0, bytes_accessed=100_000_000, transcendentals=0),
    )(*weights, queries, keys, values, segment[:, None], seg_row)
    return [out.reshape(count * rows, cols) for out in outs[:3]], outs[3]


def update_kernel(count, *refs):
    orders = axis_orders(count)
    bits = count.bit_length() - 1
    hiddens, tokens = refs[:3], (refs[3], refs[3], refs[4])
    olds, outs = refs[5:8], refs[8:11]
    total, staged, landed, send_sem, recv_sem = refs[11:]
    rows, cols = olds[0].shape
    me = lax.axis_index("tok")
    own = [block_of(me, orders[m]) for m in range(3)]
    copies = {}

    def first_kept(m, step):
        size = count >> (step + 1)
        return lax.div(own[m], jnp.int32(size)) * size

    def half_start(m):
        return lax.div(own[m], jnp.int32(count // 2)) * (count // 2)

    def gradient(m, block, store):
        lead = count // 2 * rows
        chunk = 128
        each = chunk // rows
        lanes = pl.ds(pl.multiple_of(lax.div(block * rows, FAST_HID) * cols, cols), cols)
        wide = tokens[m][:, lanes]

        def one(i, carry):
            at = pl.ds(pl.multiple_of(block * rows + i * chunk, chunk), chunk)
            part = jnp.dot(hiddens[m][at, :], wide, preferred_element_type=jnp.float32)
            store(i * each, each, part.reshape(each, rows, cols))
            return carry

        lax.fori_loop(0, lead // chunk, one, 0)

    def stage_first(m, at, size, part):
        staged[m, pl.ds(at, size)] = part.astype(jnp.bfloat16)

    def keep_first(m, at, size, part):
        total[m, pl.ds(at, size)] = part

    def send_half(m, step):
        bit = orders[m][step]
        size = count >> (step + 1)
        place = pl.ds(count - 2 * size, size)
        copies[m, step] = remote(
            staged.at[m, place],
            landed.at[m, place],
            send_sem.at[m, step],
            recv_sem.at[m, step],
            partner_of(me, bit, bits),
        )
        copies[m, step].start()

    def pass_on(m, step):
        size = count >> (step + 1)
        base, keep = first_kept(m, step - 1), first_kept(m, step)
        away = 2 * base + size - keep
        half = half_start(m)
        below = count - 4 * size

        def sum_of(block):
            other = landed[m, below + block - base].astype(jnp.float32)
            return total[m, block - half] + other

        def stage(i, carry):
            staged[m, count - 2 * size + i] = sum_of(away + i).astype(jnp.bfloat16)
            return carry

        def hold(i, carry):
            total[m, keep - half + i] = sum_of(keep + i)
            return carry

        lax.fori_loop(0, size, stage, 0)
        send_half(m, step)
        lax.fori_loop(0, size, hold, 0)

    def send_new(m, step):
        bit = orders[m][bits - 1 - step]
        size = 1 << step
        start = lax.div(own[m], jnp.int32(size)) * size
        here = outs[m].at[pl.ds(start, size)]
        at = bits + step
        copies[m, at] = remote(
            here, here, send_sem.at[m, at], recv_sem.at[m, at], partner_of(me, bit, bits)
        )
        copies[m, at].start()

    for m in range(3):
        gradient(m, count // 2 - half_start(m), functools.partial(stage_first, m))
        if m == 0:
            greet(me, bits)
        send_half(m, 0)
    for m in range(3):
        gradient(m, half_start(m), functools.partial(keep_first, m))
    for step in range(1, bits):
        for m in range(3):
            copies[m, step - 1].wait_recv()
            pass_on(m, step)
    for m in range(3):
        copies[m, bits - 1].wait_recv()
        grad = total[m, own[m] - half_start(m)] + landed[m, count - 2].astype(jnp.float32)
        old = olds[m][...].astype(jnp.float32)
        update = old - grad
        old_len = jnp.sqrt(jnp.sum(old * old, axis=1, keepdims=True))
        new_len = jnp.sqrt(jnp.sum(update * update, axis=1, keepdims=True) + EPS)
        outs[m][own[m]] = (update * (old_len / new_len)).astype(jnp.bfloat16)
        send_new(m, 0)
    for step in range(bits):
        for m in range(3):
            copies[m, bits + step].wait_recv()
            if step + 1 < bits:
                send_new(m, step + 1)
    for copy in copies.values():
        copy.wait_send()


def update_weights(hiddens, keys, values, olds, count):
    rows, cols = olds[0].shape
    bits = count.bit_length() - 1
    shape = (count, rows, cols)
    return pl.pallas_call(
        functools.partial(update_kernel, count),
        out_shape=[jax.ShapeDtypeStruct(shape, jnp.bfloat16)] * 3,
        in_specs=[pl.BlockSpec(memory_space=pltpu.VMEM)] * 8,
        out_specs=[pl.BlockSpec(memory_space=pltpu.VMEM)] * 3,
        scratch_shapes=[
            pltpu.VMEM((3, count // 2, rows, cols), jnp.float32),
            pltpu.VMEM((3, count, rows, cols), jnp.bfloat16),
            pltpu.VMEM((3, count, rows, cols), jnp.bfloat16),
            pltpu.SemaphoreType.DMA((3, 2 * bits)),
            pltpu.SemaphoreType.DMA((3, 2 * bits)),
        ],
        compiler_params=pltpu.CompilerParams(collective_id=1, has_side_effects=True),
        cost_estimate=pl.CostEstimate(flops=0, bytes_accessed=200_000_000, transcendentals=0),
    )(*hiddens, keys, values, *olds)


def project(rows, weight):
    matrix = weight.reshape(FAST_HEADS, FAST_DIM, weight.shape[1])
    return jnp.einsum("thd,hdc->thc", rows, matrix, preferred_element_type=jnp.float32)


def hidden_first(hidden):
    return hidden.astype(jnp.bfloat16).reshape(hidden.shape[0], FAST_HEADS * FAST_HID).T


def per_device(queries, keys, values, segment, rates, fast_one, fast_three, fast_two):
    count = queries.shape[0]
    devices = lax.axis_size("tok")
    shard = lax.axis_index("tok")
    width = FAST_HEADS * FAST_DIM
    key_fast = keys.reshape(count, FAST_HEADS, FAST_DIM)
    value_fast = values.reshape(count, FAST_HEADS, FAST_DIM)
    query_fast = queries.reshape(count, FAST_HEADS, FAST_DIM)
    fulls, attended = gather_weights(
        (fast_one, fast_three, fast_two), queries, keys, values, segment, devices
    )
    full_one, full_three, full_two = fulls
    rate = rates[:, :, None]
    a_one = project(key_fast, full_one)
    a_three = project(key_fast, full_three)
    sig = jax.nn.sigmoid(a_one)
    weighted = (-rate * a_one * sig * a_three).astype(jnp.bfloat16)
    back = -rate * project(value_fast, full_two)
    delta_one = (back * a_three * sig * (1.0 + a_one * (1.0 - sig))).astype(jnp.bfloat16)
    delta_three = (back * a_one * sig).astype(jnp.bfloat16)
    hiddens = [hidden_first(hidden) for hidden in (delta_one, delta_three, weighted)]
    rows_here = FAST_HEADS * FAST_HID // devices
    olds = []
    for m, order in enumerate(axis_orders(devices)):
        start = block_of(shard, order) * rows_here
        own_cols = lax.dynamic_slice(
            fulls[m].reshape(FAST_HEADS, FAST_DIM, FAST_HID),
            (start // FAST_HID, jnp.int32(0), start % FAST_HID),
            (1, FAST_DIM, rows_here),
        )
        olds.append(own_cols[0].T)
    news = update_weights(hiddens, keys, values, olds, devices)
    new_one, new_three, new_two = [n.reshape(FAST_HEADS, FAST_HID, FAST_DIM) for n in news]
    b_one = jnp.einsum("thd,hcd->thc", query_fast, new_one, preferred_element_type=jnp.float32)
    b_three = jnp.einsum("thd,hcd->thc", query_fast, new_three, preferred_element_type=jnp.float32)
    mixed = (jax.nn.silu(b_one) * b_three).astype(jnp.bfloat16)
    fast_out = jnp.einsum("thc,hcd->thd", mixed, new_two, preferred_element_type=jnp.float32)
    fast_out = fast_out.reshape(count, width).astype(jnp.bfloat16)
    return (attended, fast_out)


def solution(mesh):
    placed = (
        P(("grp", "tok"), None),
        P(("grp", "tok"), None),
        P(("grp", "tok"), None),
        P(("grp", "tok")),
        P(("grp", "tok"), None),
        P(("grp", "tok"), None),
        P(("grp", "tok"), None),
        P(("grp", "tok"), None),
    )
    return jax.shard_map(
        per_device,
        mesh=mesh,
        in_specs=placed,
        out_specs=(P(("grp", "tok"), None), P(("grp", "tok"), None)),
        check_vma=False,
    )
```

```python
import functools
import math

import jax
import jax.numpy as jnp
from jax import lax
from jax.experimental import pallas as pl
from jax.experimental.pallas import tpu as pltpu
from jax.sharding import PartitionSpec as P

D = 2048
ATT_HEADS = 16
FAST_HEADS = 2
FAST_DIM = 1024
FAST_HID = 512
WINDOW = 128


EPS = 1e-06


def axis_orders(count):
    bits = count.bit_length() - 1
    rest = list(range(1, bits))
    return [[0] + rest[m:] + rest[:m] if rest else [0] for m in range(3)]


def bit_of(index, bit):
    return lax.rem(lax.div(index, jnp.int32(1 << bit)), jnp.int32(2))


def coordinate(index, bit, bits):
    here = bit_of(index, bit)
    if bits >= 3 and bit == bits - 2:
        top = bit_of(index, bits - 1)
        here = here + top - 2 * here * top
    return here


def partner_of(me, bit, bits):
    other = me + (1 - 2 * bit_of(me, bit)) * (1 << bit)
    if bits >= 3 and bit == bits - 1:
        other = other + (1 - 2 * bit_of(me, bit - 1)) * (1 << (bit - 1))
    return other


def block_of(index, order):
    total = jnp.int32(0)
    for bit in order:
        total = total * 2 + coordinate(index, bit, len(order))
    return total


def device_of(block, order):
    bits = len(order)
    index = 0
    for place, bit in enumerate(reversed(order)):
        index += ((block >> place) & 1) << bit
    if bits >= 3 and (index >> (bits - 1)) & 1:
        index ^= 1 << (bits - 2)
    return index


def greet(me, bits, others=()):
    barrier = pltpu.get_barrier_semaphore()
    partners = [partner_of(me, bit, bits) for bit in range(bits)] + list(others)
    for partner in partners:
        pl.semaphore_signal(
            barrier,
            inc=1,
            device_id={"tok": partner},
            device_id_type=pl.DeviceIdType.MESH,
        )
    pl.semaphore_wait(barrier, len(partners))


def remote(src, dst, send_sem, recv_sem, partner):
    return pltpu.make_async_remote_copy(
        src_ref=src,
        dst_ref=dst,
        send_sem=send_sem,
        recv_sem=recv_sem,
        device_id={"tok": partner},
        device_id_type=pl.DeviceIdType.MESH,
    )


def gather_kernel(count, *refs):
    orders = axis_orders(count)
    bits = count.bit_length() - 1
    parts = refs[:3]
    q_ref, k_ref, v_ref, seg_col, seg_row = refs[3:8]
    outs, att_ref = refs[8:11], refs[11]
    held, old_k, old_v, old_seg, local_sem, send_sem, recv_sem, halo_send, halo_recv = refs[12:]
    me = lax.axis_index("tok")
    after, before = lax.rem(me + 1, count), lax.rem(me + count - 1, count)
    own = [block_of(me, orders[m]) for m in range(3)]
    local = [
        pltpu.make_async_copy(parts[m], held.at[m, own[m]], local_sem.at[m]) for m in range(3)
    ]
    for copy in local:
        copy.start()
    greet(me, bits, (after, before))
    copies = {}

    def send(m, step):
        bit = orders[m][bits - 1 - step]
        size = 1 << step
        start = lax.div(own[m], jnp.int32(size)) * size
        here = held.at[m, pl.ds(start, size)]
        copies[m, step] = remote(
            here, here, send_sem.at[m, step], recv_sem.at[m, step], partner_of(me, bit, bits)
        )
        copies[m, step].start()

    for m in range(3):
        local[m].wait()
        send(m, 0)
    halo = [
        remote(src, dst, halo_send.at[i], halo_recv.at[i], after)
        for i, (src, dst) in enumerate(((seg_row, old_seg), (k_ref, old_k), (v_ref, old_v)))
    ]
    for copy in halo:
        copy.start()

    rows = q_ref.shape[0]
    dim = D // ATT_HEADS
    scale = 1.0 / math.sqrt(dim)

    def attend_heads(first, last):
        row = lax.broadcasted_iota(jnp.int32, (rows, rows), 0)
        col = lax.broadcasted_iota(jnp.int32, (rows, rows), 1)
        own_seg = seg_col[...]
        now_ok = (col <= row) & (row - col < WINDOW) & (own_seg == seg_row[0:1, :])
        old_ok = (row - col + rows < WINDOW) & (own_seg == old_seg[0:1, :]) & (row + me * rows >= row + rows)

        def one(head, carry):
            lanes = pl.ds(pl.multiple_of(head * dim, dim), dim)
            q = q_ref[:, lanes]

            def score(keys, allowed):
                dots = lax.dot_general(
                    q, keys, (((1,), (1,)), ((), ())), preferred_element_type=jnp.float32
                )
                return jnp.where(allowed, dots * scale, jnp.float32(-1e30))

            old, now = score(old_k[:, lanes], old_ok), score(k_ref[:, lanes], now_ok)
            top = jnp.maximum(
                jnp.max(old, axis=1, keepdims=True), jnp.max(now, axis=1, keepdims=True)
            )
            old = jnp.where(old_ok, jnp.exp(old - top), jnp.float32(0.0))
            now = jnp.where(now_ok, jnp.exp(now - top), jnp.float32(0.0))
            total = jnp.sum(old, axis=1, keepdims=True) + jnp.sum(now, axis=1, keepdims=True)
            out = jnp.dot(
                (old / total).astype(jnp.bfloat16),
                old_v[:, lanes],
                preferred_element_type=jnp.float32,
            ) + jnp.dot(
                (now / total).astype(jnp.bfloat16),
                v_ref[:, lanes],
                preferred_element_type=jnp.float32,
            )
            att_ref[:, lanes] = out.astype(jnp.bfloat16)
            return carry

        lax.fori_loop(first, last, one, 0)

    for step in range(bits):
        if step == bits - 2:
            for copy in halo:
                copy.wait_recv()
            attend_heads(0, 12)
        if step == bits - 1:
            attend_heads(12, ATT_HEADS)
        for m in range(3):
            copies[m, step].wait_recv()
            if step + 1 < bits:
                send(m, step + 1)
            else:
                for block in range(count):
                    outs[m][device_of(block, orders[m])] = held[m, block]
    for copy in list(copies.values()) + halo:
        copy.wait_send()


def gather_weights(weights, queries, keys, values, segment, count):
    rows, cols = weights[0].shape
    tokens = queries.shape[0]
    bits = count.bit_length() - 1
    seg_row = jnp.broadcast_to(segment[None, :], (8, tokens))
    outs = pl.pallas_call(
        functools.partial(gather_kernel, count),
        out_shape=[jax.ShapeDtypeStruct((count, rows, cols), jnp.bfloat16)] * 3
        + [jax.ShapeDtypeStruct(queries.shape, jnp.bfloat16)],
        in_specs=[pl.BlockSpec(memory_space=pltpu.VMEM)] * 8,
        out_specs=[pl.BlockSpec(memory_space=pltpu.VMEM)] * 4,
        scratch_shapes=[
            pltpu.VMEM((3, count, rows, cols), jnp.bfloat16),
            pltpu.VMEM(keys.shape, jnp.bfloat16),
            pltpu.VMEM(values.shape, jnp.bfloat16),
            pltpu.VMEM((8, tokens), jnp.int32),
            pltpu.SemaphoreType.DMA((3,)),
            pltpu.SemaphoreType.DMA((3, bits)),
            pltpu.SemaphoreType.DMA((3, bits)),
            pltpu.SemaphoreType.DMA((3,)),
            pltpu.SemaphoreType.DMA((3,)),
        ],
        compiler_params=pltpu.CompilerParams(collective_id=0, has_side_effects=True),
        cost_estimate=pl.CostEstimate(flops=0, bytes_accessed=100_000_000, transcendentals=0),
    )(*weights, queries, keys, values, segment[:, None], seg_row)
    return [out.reshape(count * rows, cols) for out in outs[:3]], outs[3]


def update_kernel(count, *refs):
    orders = axis_orders(count)
    bits = count.bit_length() - 1
    hiddens, tokens = refs[:3], (refs[3], refs[3], refs[4])
    olds, outs = refs[5:8], refs[8:11]
    total, staged, landed, send_sem, recv_sem = refs[11:]
    rows, cols = olds[0].shape
    me = lax.axis_index("tok")
    own = [block_of(me, orders[m]) for m in range(3)]
    copies = {}

    def first_kept(m, step):
        size = count >> (step + 1)
        return lax.div(own[m], jnp.int32(size)) * size

    def half_start(m):
        return lax.div(own[m], jnp.int32(count // 2)) * (count // 2)

    def gradient(m, block, store):
        lead = count // 2 * rows
        chunk = 128
        each = chunk // rows
        lanes = pl.ds(pl.multiple_of(lax.div(block * rows, FAST_HID) * cols, cols), cols)
        wide = tokens[m][:, lanes]

        def one(i, carry):
            at = pl.ds(pl.multiple_of(block * rows + i * chunk, chunk), chunk)
            part = jnp.dot(hiddens[m][at, :], wide, preferred_element_type=jnp.float32)
            store(i * each, each, part.reshape(each, rows, cols))
            return carry

        lax.fori_loop(0, lead // chunk, one, 0)

    def stage_first(m, at, size, part):
        staged[m, pl.ds(at, size)] = part.astype(jnp.bfloat16)

    def keep_first(m, at, size, part):
        total[m, pl.ds(at, size)] = part

    def send_half(m, step):
        bit = orders[m][step]
        size = count >> (step + 1)
        place = pl.ds(count - 2 * size, size)
        copies[m, step] = remote(
            staged.at[m, place],
            landed.at[m, place],
            send_sem.at[m, step],
            recv_sem.at[m, step],
            partner_of(me, bit, bits),
        )
        copies[m, step].start()

    def pass_on(m, step):
        size = count >> (step + 1)
        base, keep = first_kept(m, step - 1), first_kept(m, step)
        away = 2 * base + size - keep
        half = half_start(m)
        below = count - 4 * size

        def sum_of(block):
            other = landed[m, below + block - base].astype(jnp.float32)
            return total[m, block - half] + other

        def stage(i, carry):
            staged[m, count - 2 * size + i] = sum_of(away + i).astype(jnp.bfloat16)
            return carry

        def hold(i, carry):
            total[m, keep - half + i] = sum_of(keep + i)
            return carry

        lax.fori_loop(0, size, stage, 0)
        send_half(m, step)
        lax.fori_loop(0, size, hold, 0)

    def send_new(m, step):
        bit = orders[m][bits - 1 - step]
        size = 1 << step
        start = lax.div(own[m], jnp.int32(size)) * size
        here = outs[m].at[pl.ds(start, size)]
        at = bits + step
        copies[m, at] = remote(
            here, here, send_sem.at[m, at], recv_sem.at[m, at], partner_of(me, bit, bits)
        )
        copies[m, at].start()

    for m in range(3):
        gradient(m, count // 2 - half_start(m), functools.partial(stage_first, m))
        if m == 0:
            greet(me, bits)
        send_half(m, 0)
    for m in range(3):
        gradient(m, half_start(m), functools.partial(keep_first, m))
    for step in range(1, bits):
        for m in range(3):
            copies[m, step - 1].wait_recv()
            pass_on(m, step)
    for m in range(3):
        copies[m, bits - 1].wait_recv()
        grad = total[m, own[m] - half_start(m)] + landed[m, count - 2].astype(jnp.float32)
        old = olds[m][...].astype(jnp.float32)
        update = old - grad
        old_len = jnp.sqrt(jnp.sum(old * old, axis=1, keepdims=True))
        new_len = jnp.sqrt(jnp.sum(update * update, axis=1, keepdims=True) + EPS)
        outs[m][own[m]] = (update * (old_len / new_len)).astype(jnp.bfloat16)
        send_new(m, 0)
    for step in range(bits):
        for m in range(3):
            copies[m, bits + step].wait_recv()
            if step + 1 < bits:
                send_new(m, step + 1)
    for copy in copies.values():
        copy.wait_send()


def update_weights(hiddens, keys, values, olds, count):
    rows, cols = olds[0].shape
    bits = count.bit_length() - 1
    shape = (count, rows, cols)
    return pl.pallas_call(
        functools.partial(update_kernel, count),
        out_shape=[jax.ShapeDtypeStruct(shape, jnp.bfloat16)] * 3,
        in_specs=[pl.BlockSpec(memory_space=pltpu.VMEM)] * 8,
        out_specs=[pl.BlockSpec(memory_space=pltpu.VMEM)] * 3,
        scratch_shapes=[
            pltpu.VMEM((3, count // 2, rows, cols), jnp.float32),
            pltpu.VMEM((3, count, rows, cols), jnp.bfloat16),
            pltpu.VMEM((3, count, rows, cols), jnp.bfloat16),
            pltpu.SemaphoreType.DMA((3, 2 * bits)),
            pltpu.SemaphoreType.DMA((3, 2 * bits)),
        ],
        compiler_params=pltpu.CompilerParams(collective_id=1, has_side_effects=True),
        cost_estimate=pl.CostEstimate(flops=0, bytes_accessed=200_000_000, transcendentals=0),
    )(*hiddens, keys, values, *olds)


def project(rows, weight):
    matrix = weight.reshape(FAST_HEADS, FAST_DIM, weight.shape[1])
    return jnp.einsum("thd,hdc->thc", rows, matrix, preferred_element_type=jnp.float32)


def hidden_first(hidden):
    return hidden.astype(jnp.bfloat16).reshape(hidden.shape[0], FAST_HEADS * FAST_HID).T


def per_device(queries, keys, values, segment, rates, fast_one, fast_three, fast_two):
    count = queries.shape[0]
    devices = lax.axis_size("tok")
    shard = lax.axis_index("tok")
    width = FAST_HEADS * FAST_DIM
    key_fast = keys.reshape(count, FAST_HEADS, FAST_DIM)
    value_fast = values.reshape(count, FAST_HEADS, FAST_DIM)
    query_fast = queries.reshape(count, FAST_HEADS, FAST_DIM)
    fulls, attended = gather_weights(
        (fast_one, fast_three, fast_two), queries, keys, values, segment, devices
    )
    full_one, full_three, full_two = fulls
    rate = rates[:, :, None]
    a_one = project(key_fast, full_one)
    a_three = project(key_fast, full_three)
    sig = jax.nn.sigmoid(a_one)
    weighted = (-rate * a_one * sig * a_three).astype(jnp.bfloat16)
    back = -rate * project(value_fast, full_two)
    delta_one = (back * a_three * sig * (1.0 + a_one * (1.0 - sig))).astype(jnp.bfloat16)
    delta_three = (back * a_one * sig).astype(jnp.bfloat16)
    hiddens = [hidden_first(hidden) for hidden in (delta_one, delta_three, weighted)]
    rows_here = FAST_HEADS * FAST_HID // devices
    olds = []
    for m, order in enumerate(axis_orders(devices)):
        start = block_of(shard, order) * rows_here
        own_cols = lax.dynamic_slice(
            fulls[m].reshape(FAST_HEADS, FAST_DIM, FAST_HID),
            (start // FAST_HID, jnp.int32(0), start % FAST_HID),
            (1, FAST_DIM, rows_here),
        )
        olds.append(own_cols[0].T)
    news = update_weights(hiddens, keys, values, olds, devices)
    new_one, new_three, new_two = [n.reshape(FAST_HEADS, FAST_HID, FAST_DIM) for n in news]
    b_one = jnp.einsum("thd,hcd->thc", query_fast, new_one, preferred_element_type=jnp.float32)
    b_three = jnp.einsum("thd,hcd->thc", query_fast, new_three, preferred_element_type=jnp.float32)
    mixed = (jax.nn.silu(b_one) * b_three).astype(jnp.bfloat16)
    fast_out = jnp.einsum("thc,hcd->thd", mixed, new_two, preferred_element_type=jnp.float32)
    fast_out = fast_out.reshape(count, width).astype(jnp.bfloat16)
    return (attended, fast_out)


def solution(mesh):
    placed = (
        P(("grp", "tok"), None),
        P(("grp", "tok"), None),
        P(("grp", "tok"), None),
        P(("grp", "tok")),
        P(("grp", "tok"), None),
        P(("grp", "tok"), None),
        P(("grp", "tok"), None),
        P(("grp", "tok"), None),
    )
    return jax.shard_map(
        per_device,
        mesh=mesh,
        in_specs=placed,
        out_specs=(P(("grp", "tok"), None), P(("grp", "tok"), None)),
        check_vma=False,
    )
```
